32 devices in a mesh: seq: 8 (over y, x, core), head: 4 (over z).
Axes of the slice: x: 2, y: 2, z: 4, core: 2. Of those that a mesh axis runs over, the one named last changes fastest.
Arguments:
- q_values: bfloat16 [16384, 4096], P('seq', 'head'), may hold values from -6 to 6
- k_values: bfloat16 [16384, 4096], P('seq', 'head'), may hold values from -6 to 6
- v_values: bfloat16 [16384, 4096], P('seq', 'head'), may hold values from -6 to 6
- q_scales: float32 [16384, 32], P('seq', 'head'), may hold values from 0.5 to 4
- k_scales: float32 [16384, 32], P('seq', 'head'), may hold values from 0.5 to 4
- v_scales: float32 [16384, 32], P('seq', 'head'), may hold values from 0.5 to 2
- conv_weight: float32 [32, 33], P('head'), may hold values from -0.9 to 0.9
Outputs:
- attended: bfloat16 [16384, 4096], P('seq', 'head')
The draws below stay inside these ranges and needn't reach their ends.
All inputs are finite; a program needn't handle non-finite values.
Results may differ from the reference program's by a relative error of at most 0.03.
Values may be sent and summed in bfloat16 or wider, within the bound.
No kernel may reach another device: no remote copies, remote signals or barrier semaphores. Data moves between devices by JAX's collectives and lax.ppermute only.
A program may use at most 128 MiB of HBM per device.

```python
import math
import jax
import jax.numpy as jnp
from jax import lax

HEADS = 32
HEAD_DIM = 128
LANDMARKS = 256
CONV = 33
SWEEPS = 6
SEQ = 16384


def shaped_field(key, which):
    segment = SEQ // LANDMARKS
    own_key = jax.random.fold_in(key, which)
    noise_key, direction_key, spread_key = jax.random.split(own_key, 3)
    noise = jax.random.normal(noise_key, (LANDMARKS, segment, HEADS, HEAD_DIM), jnp.float32)
    direction = jax.random.normal(direction_key, (LANDMARKS, 1, HEADS, HEAD_DIM), jnp.float32)
    spread = jnp.exp(jax.random.uniform(spread_key, (LANDMARKS, 1, HEADS, 1), jnp.float32, math.log(0.3), math.log(1.2)))
    offset = direction * spread
    field = jnp.clip(noise + offset, -6.0, 6.0)
    return field.reshape(SEQ, HEADS * HEAD_DIM).astype(jnp.bfloat16)


def draw_q_values(key, part):
    return shaped_field(key, 1)


def draw_k_values(key, part):
    return shaped_field(key, 2)


def block_levels(key, extent, pieces, smallest, top_value):
    def one(position, shards_of):
        steps = jax.random.uniform(jax.random.fold_in(jax.random.fold_in(key, 6), position), (shards_of,), jnp.float32, smallest / len(pieces), top_value / len(pieces))
        return jnp.repeat(jnp.exp(steps), extent[position] // shards_of).reshape((-1,) + (1,) * (len(extent) - position - 1))

    gain = one(*pieces[0])
    for cut in pieces[1:]:
        gain = gain * one(*cut)
    return gain


def centred(rng, dims, scale, limit, pieces=(), kind=jnp.bfloat16):
    factor_of = block_levels(rng, dims, pieces, -0.22, 0.18) if pieces else 1.0
    values = jax.random.normal(rng, dims, jnp.float32) * scale * factor_of
    return jnp.minimum(jnp.maximum(values, -limit), limit).astype(kind)


def setup_inputs(seed: int = 0) -> dict:
    seeds = jax.random.split(jax.random.key(seed), 8)
    return {
        "q_values": draw_q_values(jax.random.fold_in(seeds[7], 71), 0),
        "k_values": draw_k_values(jax.random.fold_in(seeds[7], 71), 0),
        "v_values": centred(seeds[2], (SEQ, HEADS * HEAD_DIM), 1.0, 6.0, ((0, 8), (1, 4))),
        "q_scales": jnp.clip(jnp.exp(math.log(4.0) - 2.0794415 * jax.random.uniform(seeds[3], (SEQ, HEADS), jnp.float32) ** block_levels(seeds[3], (SEQ, HEADS), ((0, 8), (1, 4)), -0.2, 0.2)), 0.5, 4.0),
        "k_scales": jnp.clip(jnp.exp(math.log(4.0) - 2.0794415 * jax.random.uniform(seeds[4], (SEQ, HEADS), jnp.float32) ** block_levels(seeds[4], (SEQ, HEADS), ((0, 8), (1, 4)), -0.2, 0.2)), 0.5, 4.0),
        "v_scales": jnp.clip(jnp.exp(math.log(2.0) - 1.3862944 * jax.random.uniform(seeds[5], (SEQ, HEADS), jnp.float32) ** block_levels(seeds[5], (SEQ, HEADS), ((0, 8), (1, 4)), -0.2, 0.2)), 0.5, 2.0),
        "conv_weight": centred(seeds[6], (HEADS, CONV), 0.15, 0.9, ((0, 4),), jnp.float32),
    }


def dequant(value_rows, scales):
    count = scales.shape[1]
    shaped = value_rows.reshape(value_rows.shape[0], count, HEAD_DIM).astype(jnp.float32)
    return (shaped * scales[:, :, None]).astype(jnp.bfloat16)


def newton(kernel, initial, right_side):
    highest = lax.Precision.HIGHEST
    eye_matrix = jnp.eye(kernel.shape[0], dtype=jnp.float32)
    iterate = initial
    for sweep in range(SWEEPS):
        product = jnp.dot(kernel, iterate, precision=highest)
        inner_term = 7.0 * eye_matrix - product
        inner_term = 15.0 * eye_matrix - jnp.dot(product, inner_term, precision=highest)
        inner_term = 13.0 * eye_matrix - jnp.dot(product, inner_term, precision=highest)
        iterate = 0.25 * jnp.dot(iterate, inner_term, precision=highest)
    return jnp.dot(iterate, right_side, precision=highest).astype(jnp.bfloat16)


def reference(q_values, k_values, v_values, q_scales, k_scales, v_scales, conv_weight):
    total_rows = q_values.shape[0]
    query_rows = dequant(q_values, q_scales)
    key_rows = dequant(k_values, k_scales)
    value_rows = dequant(v_values, v_scales)
    segment = total_rows // LANDMARKS

    def means(source):
        shaped = source.reshape(LANDMARKS, segment, HEADS, HEAD_DIM).astype(jnp.float32)
        return jnp.mean(shaped, axis=1).astype(jnp.bfloat16)

    query_landmarks = means(query_rows)
    key_landmarks = means(key_rows)
    pseudo_inverse_factor = HEAD_DIM ** -0.5
    landmark_kernel = jnp.einsum("jvc,kvc->vjk", query_landmarks.astype(jnp.float32), key_landmarks.astype(jnp.float32)) * pseudo_inverse_factor
    middle = jax.nn.softmax(landmark_kernel, axis=-1)
    col_top = jnp.max(jnp.sum(middle, axis=1))
    row_top = jnp.max(jnp.sum(middle, axis=2))
    start = jnp.swapaxes(middle, 1, 2) / (col_top * row_top)
    reach = CONV // 2

    def per_head(operands):
        query_head, key_head, value_head, middle_head, start_head, qmark_head, kmark_head, taps = operands
        distant_term = jnp.dot(qmark_head, key_head.T, preferred_element_type=jnp.float32) * pseudo_inverse_factor
        weight_matrix = jnp.exp(distant_term - jnp.max(distant_term, axis=1, keepdims=True))
        total = jnp.sum(weight_matrix, axis=1)
        summed = jnp.dot(weight_matrix.astype(jnp.bfloat16), value_head, preferred_element_type=jnp.float32)
        reduced = summed / total[:, None]
        projected_values = newton(middle_head, start_head, reduced)
        near_scores = jnp.dot(query_head, kmark_head.T, preferred_element_type=jnp.float32) * pseudo_inverse_factor
        local_term = jax.nn.softmax(near_scores, axis=-1).astype(jnp.bfloat16)
        attended = jnp.dot(local_term, projected_values, preferred_element_type=jnp.float32)
        padded = jnp.pad(value_head, ((reach, reach), (0, 0)))
        mixed = jnp.zeros((total_rows, HEAD_DIM), jnp.float32)
        for tap_index in range(CONV):
            mixed = mixed + padded[tap_index:tap_index + total_rows].astype(jnp.float32) * taps[tap_index]
        return (attended + mixed).astype(jnp.bfloat16)

    stacked = lax.map(per_head, (jnp.swapaxes(query_rows, 0, 1), jnp.swapaxes(key_rows, 0, 1), jnp.swapaxes(value_rows, 0, 1), middle, start, jnp.swapaxes(query_landmarks, 0, 1), jnp.swapaxes(key_landmarks, 0, 1), conv_weight))
    return jnp.swapaxes(stacked, 0, 1).reshape(total_rows, HEADS * HEAD_DIM)
```

```python
import functools

import jax
import jax.numpy as jnp
from jax import lax
from jax.experimental import pallas as pl
from jax.experimental.pallas import tpu as pltpu
from jax.sharding import PartitionSpec as P

HEAD_DIM = 128
LANDMARKS = 256
SWEEPS = 6
FACTOR = HEAD_DIM ** (-0.5)
LOG2E = 1.4426950408889634
EXTRA = 16
NEAR_BLOCK = 512
FINAL_BLOCK = 512


F32 = jnp.float32
BF16 = jnp.bfloat16
NT = (((1,), (1,)), ((), ()))
NN = (((1,), (0,)), ((), ()))


def cost(flops):
    return pl.CostEstimate(flops=flops, bytes_accessed=0, transcendentals=0)


def params(grid=True):
    semantics = ("arbitrary",) if grid else None
    return pltpu.CompilerParams(dimension_semantics=semantics, vmem_limit_bytes=24 << 20)


def heads_per_step(heads):
    return 2 if heads % 2 == 0 else 1


def vmem():
    return pl.BlockSpec(memory_space=pltpu.VMEM)


def matmul(a, b, dims=NN):
    return lax.dot_general(a, b, dims, preferred_element_type=F32)


def gather_list(array, axis, count, xor):
    if not xor:
        whole = lax.all_gather(array, axis, axis=0)
        return [whole[n] for n in range(count)]
    far = [array] + [
        lax.ppermute(array, axis, [(i, i ^ step) for i in range(count)])
        for step in range(2, count, 2)
    ]
    near = [lax.ppermute(item, axis, [(i, i ^ 1) for i in range(count)]) for item in far]
    return [item for pair in zip(far, near) for item in pair]


def source(here, n, xor):
    return jnp.bitwise_xor(here, n) if xor else n


def means_kernel(q_ref, k_ref, qs_ref, ks_ref, out_ref, *, segment):
    marks, tokens = out_ref.shape[1], q_ref.shape[0]
    per = q_ref.shape[1] // HEAD_DIM
    row = lax.broadcasted_iota(jnp.int32, (marks, tokens), 0)
    col = lax.broadcasted_iota(jnp.int32, (marks, tokens), 1)
    low = row * segment
    inside = (col >= low) & (col < low + segment)
    for which, (x_ref, s_ref) in enumerate(((q_ref, qs_ref), (k_ref, ks_ref))):
        for u in range(per):
            at = slice(u * HEAD_DIM, (u + 1) * HEAD_DIM)
            scale = s_ref[pl.ds(pl.program_id(0) * per + u, 1), :] * (1.0 / segment)
            weights = jnp.where(inside, scale, 0.0).astype(BF16)
            out_ref[which, :, at] = matmul(weights, x_ref[:, at]).astype(BF16)


def landmark_means(q, k, q_scale, k_scale, marks):
    tokens, width = q.shape
    heads = q_scale.shape[0]
    per = heads_per_step(heads)
    return pl.pallas_call(
        functools.partial(means_kernel, segment=tokens // marks),
        grid=(heads // per,),
        in_specs=[
            pl.BlockSpec((tokens, per * HEAD_DIM), lambda h: (0, h)),
            pl.BlockSpec((tokens, per * HEAD_DIM), lambda h: (0, h)),
            pl.BlockSpec((heads, tokens), lambda h: (0, 0)),
            pl.BlockSpec((heads, tokens), lambda h: (0, 0)),
        ],
        out_specs=pl.BlockSpec((2, marks, per * HEAD_DIM), lambda h: (0, 0, h)),
        out_shape=jax.ShapeDtypeStruct((2, marks, width), BF16),
        compiler_params=params(),
        cost_estimate=cost(30_000_000_000),
        name="means",
    )(q, k, q_scale, k_scale)


def conv_kernel(v_ref, before_ref, after_ref, scale_ref, taps_ref, out_ref, *, starts, block):
    tokens = v_ref.shape[0]
    per = v_ref.shape[1] // HEAD_DIM
    reach = before_ref.shape[0]
    window = block + 2 * reach
    edge = jnp.ones((1, reach), F32)
    rest = jnp.zeros((1, window - taps_ref.shape[1]), F32)
    for u in range(per):
        head = pl.program_id(0) * per + u
        at = slice(u * HEAD_DIM, (u + 1) * HEAD_DIM)
        there = pl.ds(pl.multiple_of(head * HEAD_DIM, HEAD_DIM), HEAD_DIM)
        taps = jnp.concatenate([taps_ref[pl.ds(head, 1), :], rest], axis=1)
        band = pltpu.roll(jnp.broadcast_to(taps, (block, window)), 0, 1, stride=1, stride_axis=0)
        scales = jnp.concatenate([edge, scale_ref[pl.ds(head, 1), :], edge], axis=1)
        for start in starts:
            low, high = start - reach, start + block + reach
            pieces = [v_ref[max(low, 0) : min(high, tokens), at]]
            if low < 0:
                pieces = [before_ref[:, there]] + pieces
            if high > tokens:
                pieces = pieces + [after_ref[:, there]]
            values = jnp.concatenate(pieces, axis=0) if len(pieces) > 1 else pieces[0]
            weights = (band * scales[:, start : start + window]).astype(BF16)
            out_ref[start : start + block, there] = matmul(weights, values).astype(BF16)


def convolve(v, before, after, scales, taps):
    tokens, width = v.shape
    heads, tap_count = taps.shape
    reach = tap_count // 2
    per = heads_per_step(heads)
    block = 256 - 2 * reach
    starts = sorted(set(range(0, tokens - block, block)) | {tokens - block})
    return pl.pallas_call(
        functools.partial(conv_kernel, starts=starts, block=block),
        grid=(heads // per,),
        in_specs=[
            pl.BlockSpec((tokens, per * HEAD_DIM), lambda h: (0, h)),
            vmem(),
            vmem(),
            pl.BlockSpec(scales.shape, lambda h: (0, 0)),
            pl.BlockSpec(taps.shape, lambda h: (0, 0)),
        ],
        out_specs=vmem(),
        out_shape=jax.ShapeDtypeStruct((tokens, width), BF16),
        compiler_params=params(),
        cost_estimate=cost(30_000_000_000),
        name="conv",
    )(v, before, after, scales, taps)


def landmark_softmax(q_marks, k_marks):
    scores = matmul(q_marks, k_marks, NT) * (FACTOR * LOG2E)
    weights = jnp.exp2(scores - jnp.max(scores, axis=1, keepdims=True))
    return weights / jnp.sum(weights, axis=1, keepdims=True)


def middle_kernel(here_ref, *refs, count, xor):
    pieces, (q_ref, k_ref, top_ref) = refs[:count], refs[count:]
    marks, width = pieces[0].shape[1:]
    for n in range(count):
        at = pl.multiple_of(source(here_ref[0], n, xor) * marks, marks)
        q_ref[pl.ds(at, marks), :] = pieces[n][0]
        k_ref[pl.ds(at, marks), :] = pieces[n][1]
    line = lax.broadcasted_iota(jnp.int32, top_ref.shape, 0)
    tops = []
    for start in range(0, width, HEAD_DIM):
        middle = landmark_softmax(
            q_ref[:, start : start + HEAD_DIM], k_ref[:, start : start + HEAD_DIM]
        )
        cols = jnp.sum(middle, axis=0, keepdims=True)
        cols = jnp.maximum(cols[:, :HEAD_DIM], cols[:, HEAD_DIM:])
        rows = jnp.max(jnp.sum(middle, axis=1, keepdims=True), axis=0, keepdims=True)
        tops.append(jnp.where(line == 0, cols, rows))
    top_ref[...] = functools.reduce(jnp.maximum, tops)


def middle_tops(here, pieces, xor):
    width = pieces[0].shape[2]
    return pl.pallas_call(
        functools.partial(middle_kernel, count=len(pieces), xor=xor),
        in_specs=[pl.BlockSpec(memory_space=pltpu.SMEM)] + [vmem()] * len(pieces),
        out_specs=[vmem()] * 3,
        out_shape=[
            jax.ShapeDtypeStruct((LANDMARKS, width), BF16),
            jax.ShapeDtypeStruct((LANDMARKS, width), BF16),
            jax.ShapeDtypeStruct((8, HEAD_DIM), F32),
        ],
        compiler_params=params(False),
        name="middle",
    )(here, *pieces)


def far_head(q_marks, keys, values, key_scale, value_scale):
    scores = matmul(q_marks, keys, NT) * (key_scale * (FACTOR * LOG2E))
    top = jnp.max(scores, axis=1, keepdims=True)
    weights = jnp.exp2(scores - top)
    total = jnp.sum(weights, axis=1, keepdims=True)
    weights = (weights * value_scale).astype(BF16)
    summed = matmul(weights, values) / total
    level = jnp.broadcast_to(top + jnp.log2(total), (LANDMARKS, HEAD_DIM))
    level = jnp.transpose(level)[:1, :]
    first = level.astype(BF16).astype(F32)
    second = (level - first).astype(BF16).astype(F32)
    third = level - first - second
    line = lax.broadcasted_iota(jnp.int32, (EXTRA, HEAD_DIM), 0)
    extra = jnp.zeros((EXTRA, HEAD_DIM), F32)
    for n, part in enumerate((first, second, third)):
        extra = jnp.where(line == 2 * n, part[:, :HEAD_DIM], extra)
        extra = jnp.where(line == 2 * n + 1, part[:, HEAD_DIM:], extra)
    return summed.astype(BF16), extra.astype(BF16)


def far_kernel(here_ref, q_ref, k_ref, v_ref, ks_ref, vs_ref, *out_refs, xor):
    step = pl.program_id(0)
    per = k_ref.shape[1] // HEAD_DIM
    results = []
    for u in range(per):
        head = source(here_ref[0], step * per + u, xor)
        at = pl.ds(pl.multiple_of(head % per * HEAD_DIM, HEAD_DIM), HEAD_DIM)
        there = pl.ds(pl.multiple_of(head * HEAD_DIM, HEAD_DIM), HEAD_DIM)
        scales = ks_ref[pl.ds(head, 1), :], vs_ref[pl.ds(head, 1), :]
        results.append(far_head(q_ref[:, there], k_ref[:, at], v_ref[:, at], *scales))
    for n, out_ref in enumerate(out_refs):

        @pl.when(step == n // per)
        def _(out_ref=out_ref, result=results[n % per]):
            out_ref[:LANDMARKS, :] = result[0]
            out_ref[LANDMARKS:, :] = result[1]


def far_pieces(here, q_marks, k, v, k_scale, v_scale, xor):
    tokens, width = k.shape
    heads = k_scale.shape[0]
    per = heads_per_step(heads)
    column = lambda g, here: (0, source(here[0] // per, g, xor))
    fixed = lambda g, here: (0, 0)
    shape = (LANDMARKS + EXTRA, HEAD_DIM)
    return pl.pallas_call(
        functools.partial(far_kernel, xor=xor),
        grid_spec=pltpu.PrefetchScalarGridSpec(
            num_scalar_prefetch=1,
            grid=(heads // per,),
            in_specs=[
                vmem(),
                pl.BlockSpec((tokens, per * HEAD_DIM), column),
                pl.BlockSpec((tokens, per * HEAD_DIM), column),
                pl.BlockSpec((heads, tokens), fixed),
                pl.BlockSpec((heads, tokens), fixed),
            ],
            out_specs=[vmem()] * heads,
        ),
        out_shape=[jax.ShapeDtypeStruct(shape, BF16)] * heads,
        compiler_params=params(),
        cost_estimate=cost(30_000_000_000),
        name="far",
    )(here, q_marks, k, v, k_scale, v_scale)


def split(x):
    high = x.astype(BF16)
    return high, (x - high.astype(F32)).astype(BF16)


def product(a, b):
    return matmul(a[0], b[0]) + (matmul(a[0], b[1]) + matmul(a[1], b[0]))


def newton_kernel(head_ref, q_ref, k_ref, *refs):
    tops, out_ref = refs[:-1], refs[-1]
    top = functools.reduce(jnp.maximum, [ref[...] for ref in tops])
    scale = jnp.max(top[0:1, :], axis=1, keepdims=True) * jnp.max(
        top[1:2, :], axis=1, keepdims=True
    )
    at = pl.ds(pl.multiple_of(head_ref[0] * HEAD_DIM, HEAD_DIM), HEAD_DIM)
    middle = landmark_softmax(q_ref[:, at], k_ref[:, at])
    iterate = jnp.transpose(middle) / scale
    middle = split(middle)
    row = lax.broadcasted_iota(jnp.int32, (LANDMARKS, LANDMARKS), 0)
    col = lax.broadcasted_iota(jnp.int32, (LANDMARKS, LANDMARKS), 1)
    eye = jnp.where(row == col, 1.0, 0.0)
    for sweep in range(SWEEPS):
        pair = split(iterate)
        whole = product(middle, pair)
        power = split(whole)
        inner = 7.0 * eye - whole
        inner = 15.0 * eye - product(power, split(inner))
        inner = 13.0 * eye - product(power, split(inner))
        iterate = 0.25 * product(pair, split(inner))
    out_ref[...] = iterate


def newton(head, q_marks, k_marks, tops):
    return pl.pallas_call(
        newton_kernel,
        in_specs=[pl.BlockSpec(memory_space=pltpu.SMEM)] + [vmem()] * (2 + len(tops)),
        out_specs=vmem(),
        out_shape=jax.ShapeDtypeStruct((LANDMARKS, LANDMARKS), F32),
        cost_estimate=cost(30_000_000_000),
        compiler_params=params(False),
        name="newton",
    )(head, q_marks, k_marks, *tops)


def apply_kernel(inverse_ref, *refs):
    pieces, out_ref = refs[:-1], refs[-1]
    count = len(pieces)
    levels = []
    for ref in pieces:
        extra = ref[LANDMARKS:, :].astype(F32)
        halves = [extra[n : n + 1] + extra[n + 2 : n + 3] + extra[n + 4 : n + 5] for n in (0, 1)]
        levels.append(jnp.concatenate(halves, axis=1))
    top = functools.reduce(jnp.maximum, levels)
    shares = [jnp.exp2(level - top) for level in levels]
    total = functools.reduce(jnp.add, shares)
    line = lax.broadcasted_iota(jnp.int32, (HEAD_DIM, LANDMARKS), 0)
    table = jnp.zeros((HEAD_DIM, LANDMARKS), F32)
    for n, share in enumerate(shares):
        table = jnp.where(line == n, share / total, table)
    table = jnp.transpose(table)
    reduced = jnp.zeros((LANDMARKS, HEAD_DIM), F32)
    for n in range(count):
        reduced = reduced + pieces[n][:LANDMARKS, :].astype(F32) * table[:, n : n + 1]
    out_ref[...] = product(split(inverse_ref[...]), split(reduced)).astype(BF16)


def apply_inverse(inverse, pieces):
    return pl.pallas_call(
        apply_kernel,
        in_specs=[vmem()] * (1 + len(pieces)),
        out_specs=vmem(),
        out_shape=jax.ShapeDtypeStruct((LANDMARKS, HEAD_DIM), BF16),
        compiler_params=params(False),
        name="apply",
    )(inverse, *pieces)


def near_kernel(q_ref, qs_ref, marks_ref, out_ref):
    heads, block = qs_ref.shape
    rows = pl.ds(pl.multiple_of(pl.program_id(0) * block, block), block)
    scales = jnp.transpose(qs_ref[...] * (FACTOR * LOG2E))
    for h in range(heads):
        at = slice(h * HEAD_DIM, (h + 1) * HEAD_DIM)
        scores = matmul(q_ref[:, at], marks_ref[:, at], NT) * scales[:, h : h + 1]
        weights = jnp.exp2(scores - jnp.max(scores, axis=1, keepdims=True))
        out_ref[rows, h * LANDMARKS : (h + 1) * LANDMARKS] = weights.astype(BF16)


def near_weights(q, q_scale, k_marks):
    tokens, width = q.shape
    heads = q_scale.shape[0]
    block = NEAR_BLOCK
    return pl.pallas_call(
        near_kernel,
        grid=(tokens // block,),
        in_specs=[
            pl.BlockSpec((block, width), lambda t: (t, 0)),
            pl.BlockSpec((heads, block), lambda t: (0, t)),
            vmem(),
        ],
        out_specs=vmem(),
        out_shape=jax.ShapeDtypeStruct((tokens, heads * LANDMARKS), BF16),
        compiler_params=params(),
        cost_estimate=cost(30_000_000_000),
        name="near",
    )(q, q_scale, k_marks)


def final_kernel(here_ref, near_ref, conv_ref, *refs, xor):
    mapped, (out_ref, table_ref) = refs[:-2], refs[-2:]
    block = out_ref.shape[0]
    rows = pl.ds(pl.multiple_of(pl.program_id(0) * block, block), block)

    @pl.when(pl.program_id(0) == 0)
    def _():
        for n, ref in enumerate(mapped):
            head = source(here_ref[0], n, xor)
            table_ref[head, :, :HEAD_DIM] = ref[...]
            table_ref[head, :, HEAD_DIM:] = jnp.ones((LANDMARKS, HEAD_DIM), BF16)

    for h in range(len(mapped)):
        at = slice(h * HEAD_DIM, (h + 1) * HEAD_DIM)
        both = matmul(near_ref[rows, h * LANDMARKS : (h + 1) * LANDMARKS], table_ref[h])
        attended = both[:, :HEAD_DIM] / both[:, HEAD_DIM:]
        out_ref[:, at] = (attended + conv_ref[rows, at].astype(F32)).astype(BF16)


def finish(here, near, conv, mapped, xor):
    tokens, width = conv.shape
    block = FINAL_BLOCK
    heads = len(mapped)
    return pl.pallas_call(
        functools.partial(final_kernel, xor=xor),
        grid=(tokens // block,),
        in_specs=[pl.BlockSpec(memory_space=pltpu.SMEM)] + [vmem()] * (2 + heads),
        out_specs=pl.BlockSpec((block, width), lambda t: (t, 0)),
        out_shape=jax.ShapeDtypeStruct((tokens, width), BF16),
        scratch_shapes=[pltpu.VMEM((heads, LANDMARKS, 2 * HEAD_DIM), BF16)],
        compiler_params=params(),
        name="finish",
    )(here, near, conv, *mapped)


def dequant(value_rows, scales):
    count = scales.shape[1]
    shaped = value_rows.reshape(value_rows.shape[0], count, HEAD_DIM).astype(F32)
    return (shaped * scales[:, :, None]).astype(BF16).reshape(value_rows.shape)


def shards(q_values, k_values, v_values, q_scales, k_scales, v_scales, conv_weight):
    tokens, width = q_values.shape
    heads, tap_count = conv_weight.shape
    reach = tap_count // 2
    seq_count, head_count = lax.axis_size("seq"), lax.axis_size("head")
    marks = LANDMARKS // seq_count
    xor = seq_count == heads and seq_count & (seq_count - 1) == 0
    position = lax.axis_index("seq").astype(jnp.int32)
    here = position.reshape(1)

    up = [(i, i + 1) for i in range(seq_count - 1)]
    down = [(j, i) for i, j in up]
    before = lax.ppermute(dequant(v_values[-reach:], v_scales[-reach:]), "seq", up)
    after = lax.ppermute(dequant(v_values[:reach], v_scales[:reach]), "seq", down)

    q_scale, k_scale, v_scale = q_scales.T, k_scales.T, v_scales.T
    means = landmark_means(q_values, k_values, q_scale, k_scale, marks)
    means = gather_list(means, "seq", seq_count, xor)

    mixed = convolve(v_values, before, after, v_scale, conv_weight)
    means, mixed = lax.optimization_barrier((means, mixed))

    q_marks, k_marks, top = middle_tops(here, means, xor)
    if head_count & (head_count - 1) == 0 and head_count <= 4:
        tops = [top] + [
            lax.ppermute(top, "head", [(i, i ^ step) for i in range(head_count)])
            for step in range(1, head_count)
        ]
    else:
        tops = [lax.pmax(top, "head")]

    pieces = far_pieces(here, q_marks, k_values, v_values, k_scale, v_scale, xor)
    if xor:
        own_head = here
        pieces = [pieces[0]] + [
            lax.ppermute(pieces[step], "seq", [(i, i ^ step) for i in range(seq_count)])
            for step in range(1, seq_count)
        ]
    else:
        repeat = seq_count // heads
        own_head = here // repeat
        whole = lax.all_gather(jnp.stack(pieces), "seq", axis=0)
        mine = lax.dynamic_index_in_dim(whole, own_head[0], axis=1, keepdims=False)
        pieces = [mine[n] for n in range(seq_count)]

    inverse = newton(own_head, q_marks, k_marks, tops)
    mapped = apply_inverse(inverse, pieces)
    mapped = gather_list(mapped, "seq", seq_count, xor)
    if not xor:
        mapped = mapped[:: seq_count // heads]
    near = near_weights(q_values, q_scale, k_marks)
    return finish(here, near, mixed, mapped, xor)


def solution(mesh):
    return jax.shard_map(
        shards,
        mesh=mesh,
        in_specs=(
            P("seq", "head"),
            P("seq", "head"),
            P("seq", "head"),
            P("seq", "head"),
            P("seq", "head"),
            P("seq", "head"),
            P("head", None),
        ),
        out_specs=P("seq", "head"),
        check_vma=False,
    )
```

```python
import functools

import jax
import jax.numpy as jnp
from jax import lax
from jax.experimental import pallas as pl
from jax.experimental.pallas import tpu as pltpu
from jax.sharding import PartitionSpec as P

HEAD_DIM = 128
LANDMARKS = 256
SWEEPS = 6
FACTOR = HEAD_DIM ** (-0.5)
LOG2E = 1.4426950408889634
EXTRA = 16
COARSE = 3
NEAR_BLOCK = 512
FINAL_BLOCK = 512
MEANS_LIMIT = 44
CONV_LIMIT = 24


F32 = jnp.float32
BF16 = jnp.bfloat16
NT = (((1,), (1,)), ((), ()))
NN = (((1,), (0,)), ((), ()))


def cost(flops):
    return pl.CostEstimate(flops=flops, bytes_accessed=0, transcendentals=0)


def params(grid=True, limit=24):
    semantics = ("arbitrary",) if grid else None
    return pltpu.CompilerParams(dimension_semantics=semantics, vmem_limit_bytes=limit << 20)


def heads_per_step(heads):
    return 2 if heads % 2 == 0 else 1


def vmem():
    return pl.BlockSpec(memory_space=pltpu.VMEM)


def matmul(a, b, dims=NN):
    return lax.dot_general(a, b, dims, preferred_element_type=F32)


def exchange_far(array, axis, count):
    return [
        lax.ppermute(array, axis, [(i, i ^ step) for i in range(count)])
        for step in range(2, count, 2)
    ]


def exchange_near(items, axis, count):
    return [lax.ppermute(item, axis, [(i, i ^ 1) for i in range(count)]) for item in items]


def interleave(first, second):
    return [item for pair in zip(first, second) for item in pair]


def gather_all(array, axis, count):
    whole = lax.all_gather(array, axis, axis=0)
    return [whole[n] for n in range(count)]


def source(here, n, xor):
    return jnp.bitwise_xor(here, n) if xor else n


def means_kernel(here_ref, q_ref, k_ref, head_ref, tail_ref, scale_ref, *out_refs, segment, xor):
    far_ref, near_ref, q_keep_ref, k_keep_ref = out_refs
    tokens, reach = q_ref.shape[0], head_ref.shape[0]
    marks = tokens // segment
    per = q_ref.shape[1] // HEAD_DIM
    heads = scale_ref.shape[0] // 3
    odd = here_ref[0] % 2 == 1 if xor else False
    columns = pl.ds(pl.multiple_of(pl.program_id(0) * per * HEAD_DIM, HEAD_DIM), per * HEAD_DIM)
    q_keep_ref[:, columns] = q_ref[...]
    k_keep_ref[:, columns] = k_ref[...]
    row = lax.broadcasted_iota(jnp.int32, (reach, reach), 0)
    col = lax.broadcasted_iota(jnp.int32, (reach, reach), 1)
    line = lax.broadcasted_iota(jnp.int32, (marks, tokens), 0)
    token = lax.broadcasted_iota(jnp.int32, (marks, tokens), 1)
    low = line * segment
    inside = (token >= low) & (token < low + segment)
    for u in range(per):
        head = pl.program_id(0) * per + u
        at = slice(u * HEAD_DIM, (u + 1) * HEAD_DIM)
        there = pl.ds(pl.multiple_of(head * HEAD_DIM, HEAD_DIM), HEAD_DIM)
        for which, x_ref in enumerate((q_ref, k_ref)):
            scale = scale_ref[pl.ds(which * heads + head, 1), :] * (1.0 / segment)
            weights = jnp.where(inside, scale, 0.0).astype(BF16)
            means = matmul(weights, x_ref[:, at]).astype(BF16)
            far_ref[which * marks : (which + 1) * marks, there] = means
            near_ref[which * marks : (which + 1) * marks, there] = means
        scale = scale_ref[pl.ds(2 * heads + head, 1), :]
        edges = []
        for x_ref, start in ((head_ref, 0), (tail_ref, tokens - reach)):
            diagonal = jnp.where(row == col, scale[:, start : start + reach], 0.0)
            edges.append(matmul(diagonal.astype(BF16), x_ref[:, there]))
        far_ref[2 * marks :, there] = jnp.where(odd, edges[1], edges[0]).astype(BF16)
        near_ref[2 * marks :, there] = jnp.where(odd, edges[0], edges[1]).astype(BF16)


def landmark_means(here, q, k, v, scales, marks, reach, xor):
    tokens, width = q.shape
    heads = scales.shape[0] // 3
    per = heads_per_step(heads)
    tail = tokens // reach - 1
    column = pl.BlockSpec((tokens, per * HEAD_DIM), lambda h, here: (0, h))
    payload = jax.ShapeDtypeStruct((2 * marks + reach, width), BF16)
    keep = jax.ShapeDtypeStruct((tokens, width), BF16)
    return pl.pallas_call(
        functools.partial(means_kernel, segment=tokens // marks, xor=xor),
        grid_spec=pltpu.PrefetchScalarGridSpec(
            num_scalar_prefetch=1,
            grid=(heads // per,),
            in_specs=[
                column,
                column,
                pl.BlockSpec((reach, width), lambda h, here: (0, 0)),
                pl.BlockSpec((reach, width), lambda h, here: (tail, 0)),
                vmem(),
            ],
            out_specs=[vmem()] * 4,
        ),
        out_shape=[payload, payload, keep, keep],
        compiler_params=params(limit=MEANS_LIMIT),
        cost_estimate=cost(30_000_000_000),
        name="means",
    )(here, q, k, v, v, scales)


def conv_kernel(v_ref, scale_ref, taps_ref, out_ref, keep_ref, *, starts, block):
    tokens = v_ref.shape[0]
    per = v_ref.shape[1] // HEAD_DIM
    reach = taps_ref.shape[1] // 2
    window = block + 2 * reach
    edge = jnp.zeros((1, reach), F32)
    blank = jnp.zeros((reach, HEAD_DIM), BF16)
    rest = jnp.zeros((1, window - taps_ref.shape[1]), F32)
    for u in range(per):
        head = pl.program_id(0) * per + u
        at = slice(u * HEAD_DIM, (u + 1) * HEAD_DIM)
        there = pl.ds(pl.multiple_of(head * HEAD_DIM, HEAD_DIM), HEAD_DIM)
        keep_ref[:, there] = v_ref[:, at]
        taps = jnp.concatenate([taps_ref[pl.ds(head, 1), :], rest], axis=1)
        band = pltpu.roll(jnp.broadcast_to(taps, (block, window)), 0, 1, stride=1, stride_axis=0)
        scales = jnp.concatenate([edge, scale_ref[pl.ds(scale_ref.shape[0] // 3 * 2 + head, 1), :], edge], axis=1)
        for start in starts:
            low, high = start - reach, start + block + reach
            pieces = [v_ref[max(low, 0) : min(high, tokens), at]]
            if low < 0:
                pieces = [blank] + pieces
            if high > tokens:
                pieces = pieces + [blank]
            values = jnp.concatenate(pieces, axis=0) if len(pieces) > 1 else pieces[0]
            weights = (band * scales[:, start : start + window]).astype(BF16)
            out_ref[start : start + block, there] = matmul(weights, values).astype(BF16)


def convolve(v, scales, taps):
    tokens, width = v.shape
    heads, tap_count = taps.shape
    reach = tap_count // 2
    per = heads_per_step(heads)
    block = 256 - 2 * reach
    starts = sorted(set(range(0, tokens - block, block)) | {tokens - block})
    return pl.pallas_call(
        functools.partial(conv_kernel, starts=starts, block=block),
        grid=(heads // per,),
        in_specs=[
            pl.BlockSpec((tokens, per * HEAD_DIM), lambda h: (0, h)),
            vmem(),
            vmem(),
        ],
        out_specs=[vmem()] * 2,
        out_shape=[jax.ShapeDtypeStruct((tokens, width), BF16)] * 2,
        compiler_params=params(limit=CONV_LIMIT),
        cost_estimate=cost(30_000_000_000),
        name="conv",
    )(v, scales, taps)


def landmark_softmax(q_marks, k_marks):
    scores = matmul(q_marks, k_marks, NT) * (FACTOR * LOG2E)
    weights = jnp.exp2(scores - jnp.max(scores, axis=1, keepdims=True))
    return weights / jnp.sum(weights, axis=1, keepdims=True)


def middle_kernel(here_ref, taps_ref, *refs, count, xor):
    pieces, (q_ref, k_ref, top_ref, before_ref, after_ref) = refs[:-5], refs[-5:]
    heads, tap_count = taps_ref.shape
    reach = tap_count // 2
    marks = (pieces[0].shape[0] - reach) // 2
    here = here_ref[0]
    for n in range(count):
        at = pl.multiple_of(source(here, n, xor) * marks, marks)
        q_ref[pl.ds(at, marks), :] = pieces[n][:marks, :]
        k_ref[pl.ds(at, marks), :] = pieces[n][marks : 2 * marks, :]
    line = lax.broadcasted_iota(jnp.int32, top_ref.shape, 0)
    rest = jnp.zeros((1, HEAD_DIM - tap_count), F32)
    odd = here % 2 == 1
    beyond = jnp.bitwise_xor(here, jnp.where(odd, here + 1, here - 1))
    tops = []
    for h in range(heads):
        at = slice(h * HEAD_DIM, (h + 1) * HEAD_DIM)
        middle = landmark_softmax(q_ref[:, at], k_ref[:, at])
        cols = jnp.sum(middle, axis=0, keepdims=True)
        cols = jnp.maximum(cols[:, :HEAD_DIM], cols[:, HEAD_DIM:])
        rows = jnp.max(jnp.sum(middle, axis=1, keepdims=True), axis=0, keepdims=True)
        tops.append(jnp.where(line == 0, cols, rows))
        if xor:
            beside = pieces[1][2 * marks :, at].astype(F32)
            across = jnp.zeros_like(beside)
            step = 4
            while step <= count:
                item = pieces[step - 1][2 * marks :, at].astype(F32)
                across = jnp.where(beyond == step - 1, item, across)
                step *= 2
            before = jnp.where(odd, beside, across).astype(BF16)
            after = jnp.where(odd, across, beside).astype(BF16)
        else:
            before, after = pieces[count][0, :, at], pieces[count][1, :, at]
        taps = jnp.concatenate([taps_ref[h : h + 1, :], rest], axis=1)
        band = jnp.broadcast_to(taps, (reach, HEAD_DIM))
        band = pltpu.roll(band, 0, 1, stride=1, stride_axis=0)
        low = band[:, :reach].astype(BF16)
        high = band[:, 2 * reach : 3 * reach].astype(BF16)
        before_ref[:, at] = matmul(low, before)
        after_ref[:, at] = matmul(high, after)
    top_ref[...] = functools.reduce(jnp.maximum, tops)


def middle_tops(here, taps, pieces, xor):
    width = pieces[0].shape[1]
    marks = jax.ShapeDtypeStruct((LANDMARKS, width), BF16)
    edge = jax.ShapeDtypeStruct((taps.shape[1] // 2, width), F32)
    return pl.pallas_call(
        functools.partial(middle_kernel, count=len(pieces) - (not xor), xor=xor),
        in_specs=[pl.BlockSpec(memory_space=pltpu.SMEM)] + [vmem()] * (1 + len(pieces)),
        out_specs=[vmem()] * 5,
        out_shape=[marks, marks, jax.ShapeDtypeStruct((8, HEAD_DIM), F32), edge, edge],
        compiler_params=params(False),
        name="middle",
    )(here, taps, *pieces)


def far_head(q_marks, keys, values, key_scale, value_scale):
    scores = matmul(q_marks, keys, NT) * (key_scale * (FACTOR * LOG2E))
    top = jnp.max(scores, axis=1, keepdims=True)
    weights = jnp.exp2(scores - top)
    total = jnp.sum(weights, axis=1, keepdims=True)
    weights = (weights * value_scale).astype(BF16)
    summed = matmul(weights, values) / total
    level = jnp.broadcast_to(top + jnp.log2(total), (LANDMARKS, HEAD_DIM))
    level = jnp.transpose(level)[:1, :]
    first = level.astype(BF16).astype(F32)
    second = (level - first).astype(BF16).astype(F32)
    third = level - first - second
    line = lax.broadcasted_iota(jnp.int32, (EXTRA, HEAD_DIM), 0)
    extra = jnp.zeros((EXTRA, HEAD_DIM), F32)
    for n, part in enumerate((first, second, third)):
        extra = jnp.where(line == 2 * n, part[:, :HEAD_DIM], extra)
        extra = jnp.where(line == 2 * n + 1, part[:, HEAD_DIM:], extra)
    return summed.astype(BF16), extra.astype(BF16)


def far_kernel(here_ref, q_ref, k_ref, v_ref, scale_ref, *out_refs, xor):
    step = pl.program_id(0)
    heads = scale_ref.shape[0] // 3
    per = heads_per_step(heads)
    results = []
    for u in range(per):
        head = source(here_ref[0], step * per + u, xor)
        at = pl.ds(pl.multiple_of(head * HEAD_DIM, HEAD_DIM), HEAD_DIM)
        scales = [scale_ref[pl.ds(n * heads + head, 1), :] for n in (1, 2)]
        results.append(far_head(q_ref[:, at], k_ref[:, at], v_ref[:, at], *scales))
    for n, out_ref in enumerate(out_refs):

        @pl.when(step == n // per)
        def _(out_ref=out_ref, result=results[n % per]):
            out_ref[:LANDMARKS, :] = result[0]
            out_ref[LANDMARKS:, :] = result[1]


def far_pieces(here, q_marks, k, v, scales, xor):
    heads = scales.shape[0] // 3
    per = heads_per_step(heads)
    shape = (LANDMARKS + EXTRA, HEAD_DIM)
    return pl.pallas_call(
        functools.partial(far_kernel, xor=xor),
        grid_spec=pltpu.PrefetchScalarGridSpec(
            num_scalar_prefetch=1,
            grid=(heads // per,),
            in_specs=[vmem()] * 4,
            out_specs=[vmem()] * heads,
        ),
        out_shape=[jax.ShapeDtypeStruct(shape, BF16)] * heads,
        compiler_params=params(),
        cost_estimate=cost(30_000_000_000),
        name="far",
    )(here, q_marks, k, v, scales)


def split(x):
    high = x.astype(BF16)
    return high, (x - high.astype(F32)).astype(BF16)


def fine(a, b):
    return matmul(a[0], b[0]) + (matmul(a[0], b[1]) + matmul(a[1], b[0]))


def newton_kernel(head_ref, q_ref, k_ref, *refs):
    tops, out_ref = refs[:-1], refs[-1]
    top = functools.reduce(jnp.maximum, [ref[...] for ref in tops])
    scale = jnp.max(top[0:1, :], axis=1, keepdims=True) * jnp.max(
        top[1:2, :], axis=1, keepdims=True
    )
    at = pl.ds(pl.multiple_of(head_ref[0] * HEAD_DIM, HEAD_DIM), HEAD_DIM)
    middle = landmark_softmax(q_ref[:, at], k_ref[:, at])
    iterate = jnp.transpose(middle) / scale
    middle = split(middle)
    coarse = lambda a, b: matmul(a[0], b[0])
    row = lax.broadcasted_iota(jnp.int32, (LANDMARKS, LANDMARKS), 0)
    col = lax.broadcasted_iota(jnp.int32, (LANDMARKS, LANDMARKS), 1)
    eye = jnp.where(row == col, 1.0, 0.0)
    for sweep in range(SWEEPS):
        product = coarse if sweep < COARSE else fine
        pair = split(iterate)
        whole = product(middle, pair)
        power = split(whole)
        inner = 7.0 * eye - whole
        inner = 15.0 * eye - product(power, split(inner))
        inner = 13.0 * eye - product(power, split(inner))
        iterate = 0.25 * product(pair, split(inner))
    out_ref[...] = iterate


def newton(head, q_marks, k_marks, tops):
    return pl.pallas_call(
        newton_kernel,
        in_specs=[pl.BlockSpec(memory_space=pltpu.SMEM)] + [vmem()] * (2 + len(tops)),
        out_specs=vmem(),
        out_shape=jax.ShapeDtypeStruct((LANDMARKS, LANDMARKS), F32),
        cost_estimate=cost(30_000_000_000),
        compiler_params=params(False),
        name="newton",
    )(head, q_marks, k_marks, *tops)


def apply_kernel(inverse_ref, *refs):
    pieces, out_ref = refs[:-1], refs[-1]
    count = len(pieces)
    levels = []
    for ref in pieces:
        extra = ref[LANDMARKS:, :].astype(F32)
        halves = [extra[n : n + 1] + extra[n + 2 : n + 3] + extra[n + 4 : n + 5] for n in (0, 1)]
        levels.append(jnp.concatenate(halves, axis=1))
    top = functools.reduce(jnp.maximum, levels)
    shares = [jnp.exp2(level - top) for level in levels]
    total = functools.reduce(jnp.add, shares)
    line = lax.broadcasted_iota(jnp.int32, (HEAD_DIM, LANDMARKS), 0)
    table = jnp.zeros((HEAD_DIM, LANDMARKS), F32)
    for n, share in enumerate(shares):
        table = jnp.where(line == n, share / total, table)
    table = jnp.transpose(table)
    reduced = jnp.zeros((LANDMARKS, HEAD_DIM), F32)
    for n in range(count):
        reduced = reduced + pieces[n][:LANDMARKS, :].astype(F32) * table[:, n : n + 1]
    out_ref[...] = fine(split(inverse_ref[...]), split(reduced)).astype(BF16)


def apply_inverse(inverse, pieces):
    return pl.pallas_call(
        apply_kernel,
        in_specs=[vmem()] * (1 + len(pieces)),
        out_specs=vmem(),
        out_shape=jax.ShapeDtypeStruct((LANDMARKS, HEAD_DIM), BF16),
        compiler_params=params(False),
        name="apply",
    )(inverse, *pieces)


def near_kernel(q_ref, scale_ref, marks_ref, out_ref, *, first, block):
    heads = scale_ref.shape[0] // 3
    rows = pl.ds(pl.multiple_of(pl.program_id(0) * block, block), block)
    scales = jnp.transpose(scale_ref[:heads, rows] * (FACTOR * LOG2E))
    for n in range(out_ref.shape[1] // LANDMARKS):
        at = slice((first + n) * HEAD_DIM, (first + n + 1) * HEAD_DIM)
        q = q_ref[rows, at]
        scores = matmul(q, marks_ref[:, at], NT)
        top = jnp.max(scores.astype(BF16), axis=1, keepdims=True).astype(F32)
        weights = jnp.exp2((scores - top) * scales[:, first + n : first + n + 1])
        out_ref[rows, n * LANDMARKS : (n + 1) * LANDMARKS] = weights.astype(BF16)


def near_weights(q, scales, k_marks, part, parts):
    tokens, width = q.shape
    here = scales.shape[0] // 3 // parts
    block = NEAR_BLOCK
    return pl.pallas_call(
        functools.partial(near_kernel, first=part * here, block=block),
        grid=(tokens // block,),
        in_specs=[vmem()] * 3,
        out_specs=vmem(),
        out_shape=jax.ShapeDtypeStruct((tokens, here * LANDMARKS), BF16),
        compiler_params=params(),
        cost_estimate=cost(30_000_000_000),
        name="near",
    )(q, scales, k_marks)


def final_kernel(here_ref, *refs, xor, parts):
    near, (conv_ref, before_ref, after_ref) = refs[:parts], refs[parts : parts + 3]
    mapped, (out_ref, table_ref) = refs[parts + 3 : -2], refs[-2:]
    heads = len(mapped)
    block, reach = out_ref.shape[0], before_ref.shape[0]
    step = pl.program_id(0)
    rows = pl.ds(pl.multiple_of(step * block, block), block)

    @pl.when(step == 0)
    def _():
        for n, ref in enumerate(mapped):
            head = source(here_ref[0], n, xor)
            table_ref[head, :, :HEAD_DIM] = ref[...]
            table_ref[head, :, HEAD_DIM:] = jnp.ones((LANDMARKS, HEAD_DIM), BF16)

    for h in range(heads):
        at = slice(h * HEAD_DIM, (h + 1) * HEAD_DIM)
        weights_ref = near[h * parts // heads]
        n = h % (heads // parts)
        weights = weights_ref[rows, n * LANDMARKS : (n + 1) * LANDMARKS]
        both = matmul(weights, table_ref[h])
        attended = both[:, :HEAD_DIM] / both[:, HEAD_DIM:]
        out_ref[:, at] = (attended + conv_ref[rows, at].astype(F32)).astype(BF16)

    @pl.when(step == 0)
    def _():
        out_ref[:reach, :] = (out_ref[:reach, :].astype(F32) + before_ref[...]).astype(BF16)

    @pl.when(step == pl.num_programs(0) - 1)
    def _():
        tail = slice(block - reach, block)
        out_ref[tail, :] = (out_ref[tail, :].astype(F32) + after_ref[...]).astype(BF16)


def finish(here, near, conv, before, after, mapped, xor):
    tokens, width = conv.shape
    block = FINAL_BLOCK
    heads, parts = len(mapped), len(near)
    return pl.pallas_call(
        functools.partial(final_kernel, xor=xor, parts=parts),
        grid=(tokens // block,),
        in_specs=[pl.BlockSpec(memory_space=pltpu.SMEM)] + [vmem()] * (parts + 3 + heads),
        out_specs=pl.BlockSpec((block, width), lambda t: (t, 0)),
        out_shape=jax.ShapeDtypeStruct((tokens, width), BF16),
        scratch_shapes=[pltpu.VMEM((heads, LANDMARKS, 2 * HEAD_DIM), BF16)],
        compiler_params=params(),
        name="finish",
    )(here, *near, conv, before, after, *mapped)


def shards(q_values, k_values, v_values, q_scales, k_scales, v_scales, conv_weight):
    tokens, width = q_values.shape
    heads, tap_count = conv_weight.shape
    reach = tap_count // 2
    seq_count, head_count = lax.axis_size("seq"), lax.axis_size("head")
    marks = LANDMARKS // seq_count
    xor = seq_count == heads and seq_count & (seq_count - 1) == 0
    position = lax.axis_index("seq").astype(jnp.int32)
    here = position.reshape(1)

    scales = jnp.concatenate([q_scales.T, k_scales.T, v_scales.T])
    means, means_near, q_keep, k_keep = landmark_means(
        here, q_values, k_values, v_values, scales, marks, reach, xor
    )
    mixed, v_keep = convolve(v_values, scales, conv_weight)
    if xor:
        far = exchange_far(means, "seq", seq_count)
        far, mixed = lax.optimization_barrier((far, mixed))
        near = exchange_near([means_near] + far, "seq", seq_count)
        gathered = interleave([means] + far, near)
    else:
        up = [(i, i + 1) for i in range(seq_count - 1)]
        down = [(j, i) for i, j in up]
        before = lax.ppermute(means_near[2 * marks :], "seq", up)
        after = lax.ppermute(means[2 * marks :], "seq", down)
        gathered = gather_all(means, "seq", seq_count) + [jnp.stack([before, after])]
    q_marks, k_marks, top, before, after = middle_tops(here, conv_weight, gathered, xor)
    pieces = far_pieces(here, q_marks, k_keep, v_keep, scales, xor)
    pieces, top = lax.optimization_barrier((pieces, top))
    if head_count & (head_count - 1) == 0 and head_count <= 4:
        tops = [top] + [
            lax.ppermute(top, "head", [(i, i ^ step) for i in range(head_count)])
            for step in range(1, head_count)
        ]
    else:
        tops = [lax.pmax(top, "head")]

    if xor:
        own_head = here
        pieces = [pieces[0]] + [
            lax.ppermute(pieces[step], "seq", [(i, i ^ step) for i in range(seq_count)])
            for step in range(1, seq_count)
        ]
    else:
        repeat = seq_count // heads
        own_head = here // repeat
        whole = lax.all_gather(jnp.stack(pieces), "seq", axis=0)
        mine = lax.dynamic_index_in_dim(whole, own_head[0], axis=1, keepdims=False)
        pieces = [mine[n] for n in range(seq_count)]

    inverse = newton(own_head, q_marks, k_marks, tops)
    mapped = apply_inverse(inverse, pieces)
    parts = heads_per_step(heads)
    near = [near_weights(q_keep, scales, k_marks, part, parts) for part in range(parts)]
    if xor:
        far = exchange_far(mapped, "seq", seq_count)
        far, near[0] = lax.optimization_barrier((far, near[0]))
        mapped = interleave([mapped] + far, exchange_near([mapped] + far, "seq", seq_count))
    else:
        mapped = gather_all(mapped, "seq", seq_count)[:: seq_count // heads]
    return finish(here, near, mixed, before, after, mapped, xor)


def solution(mesh):
    return jax.shard_map(
        shards,
        mesh=mesh,
        in_specs=(
            P("seq", "head"),
            P("seq", "head"),
            P("seq", "head"),
            P("seq", "head"),
            P("seq", "head"),
            P("seq", "head"),
            P("head", None),
        ),
        out_specs=P("seq", "head"),
        check_vma=False,
    )
```

```python
import functools

import jax
import jax.numpy as jnp
from jax import lax
from jax.experimental import pallas as pl
from jax.experimental.pallas import tpu as pltpu
from jax.sharding import PartitionSpec as P

HEAD_DIM = 128
LANDMARKS = 256
SWEEPS = 6
FACTOR = HEAD_DIM ** (-0.5)
LOG2E = 1.4426950408889634
EXTRA = 16
COARSE = 4
NEAR_BLOCK = 512
FINAL_BLOCK = 1024
MEANS_LIMIT = 44
CONV_LIMIT = 24


F32 = jnp.float32
BF16 = jnp.bfloat16
NT = (((1,), (1,)), ((), ()))
NN = (((1,), (0,)), ((), ()))


def cost(flops):
    return pl.CostEstimate(flops=flops, bytes_accessed=0, transcendentals=0)


def params(grid=True, limit=24):
    semantics = ("arbitrary",) if grid else None
    return pltpu.CompilerParams(dimension_semantics=semantics, vmem_limit_bytes=limit << 20)


def heads_per_step(heads):
    return 2 if heads % 2 == 0 else 1


def vmem():
    return pl.BlockSpec(memory_space=pltpu.VMEM)


def matmul(a, b, dims=NN):
    return lax.dot_general(a, b, dims, preferred_element_type=F32)


def exchange_far(array, axis, count):
    return [
        lax.ppermute(array, axis, [(i, i ^ step) for i in range(count)])
        for step in range(2, count, 2)
    ]


def exchange_near(items, axis, count):
    return [lax.ppermute(item, axis, [(i, i ^ 1) for i in range(count)]) for item in items]


def interleave(first, second):
    return [item for pair in zip(first, second) for item in pair]


def gather_all(array, axis, count):
    whole = lax.all_gather(array, axis, axis=0)
    return [whole[n] for n in range(count)]


def source(here, n, xor):
    return jnp.bitwise_xor(here, n) if xor else n


def means_kernel(here_ref, q_ref, k_ref, head_ref, tail_ref, scale_ref, *out_refs, segment, xor):
    far_ref, near_ref, q_keep_ref, k_keep_ref = out_refs
    tokens, reach = q_ref.shape[0], head_ref.shape[0]
    marks = tokens // segment
    per = q_ref.shape[1] // HEAD_DIM
    heads = scale_ref.shape[0] // 3
    odd = here_ref[0] % 2 == 1 if xor else False
    columns = pl.ds(pl.multiple_of(pl.program_id(0) * per * HEAD_DIM, HEAD_DIM), per * HEAD_DIM)
    q_keep_ref[:, columns] = q_ref[...]
    k_keep_ref[:, columns] = k_ref[...]
    row = lax.broadcasted_iota(jnp.int32, (reach, reach), 0)
    col = lax.broadcasted_iota(jnp.int32, (reach, reach), 1)
    line = lax.broadcasted_iota(jnp.int32, (marks, tokens), 0)
    token = lax.broadcasted_iota(jnp.int32, (marks, tokens), 1)
    low = line * segment
    inside = (token >= low) & (token < low + segment)
    for u in range(per):
        head = pl.program_id(0) * per + u
        at = slice(u * HEAD_DIM, (u + 1) * HEAD_DIM)
        there = pl.ds(pl.multiple_of(head * HEAD_DIM, HEAD_DIM), HEAD_DIM)
        for which, x_ref in enumerate((q_ref, k_ref)):
            scale = scale_ref[pl.ds(which * heads + head, 1), :] * (1.0 / segment)
            weights = jnp.where(inside, scale, 0.0).astype(BF16)
            means = matmul(weights, x_ref[:, at]).astype(BF16)
            far_ref[which * marks : (which + 1) * marks, there] = means
            near_ref[which * marks : (which + 1) * marks, there] = means
        scale = scale_ref[pl.ds(2 * heads + head, 1), :]
        edges = []
        for x_ref, start in ((head_ref, 0), (tail_ref, tokens - reach)):
            diagonal = jnp.where(row == col, scale[:, start : start + reach], 0.0)
            edges.append(matmul(diagonal.astype(BF16), x_ref[:, there]))
        far_ref[2 * marks :, there] = jnp.where(odd, edges[1], edges[0]).astype(BF16)
        near_ref[2 * marks :, there] = jnp.where(odd, edges[0], edges[1]).astype(BF16)


def landmark_means(here, q, k, v, scales, marks, reach, xor):
    tokens, width = q.shape
    heads = scales.shape[0] // 3
    per = heads_per_step(heads)
    tail = tokens // reach - 1
    column = pl.BlockSpec((tokens, per * HEAD_DIM), lambda h, here: (0, h))
    payload = jax.ShapeDtypeStruct((2 * marks + reach, width), BF16)
    keep = jax.ShapeDtypeStruct((tokens, width), BF16)
    return pl.pallas_call(
        functools.partial(means_kernel, segment=tokens // marks, xor=xor),
        grid_spec=pltpu.PrefetchScalarGridSpec(
            num_scalar_prefetch=1,
            grid=(heads // per,),
            in_specs=[
                column,
                column,
                pl.BlockSpec((reach, width), lambda h, here: (0, 0)),
                pl.BlockSpec((reach, width), lambda h, here: (tail, 0)),
                vmem(),
            ],
            out_specs=[vmem()] * 4,
        ),
        out_shape=[payload, payload, keep, keep],
        compiler_params=params(limit=MEANS_LIMIT),
        cost_estimate=cost(30_000_000_000),
        name="means",
    )(here, q, k, v, v, scales)


def conv_kernel(v_ref, scale_ref, taps_ref, out_ref, *, starts, block):
    tokens = v_ref.shape[0]
    per = heads_per_step(taps_ref.shape[0])
    reach = taps_ref.shape[1] // 2
    window = block + 2 * reach
    edge = jnp.zeros((1, reach), F32)
    blank = jnp.zeros((reach, HEAD_DIM), BF16)
    rest = jnp.zeros((1, window - taps_ref.shape[1]), F32)
    for u in range(per):
        head = pl.program_id(0) * per + u
        there = pl.ds(pl.multiple_of(head * HEAD_DIM, HEAD_DIM), HEAD_DIM)
        taps = jnp.concatenate([taps_ref[pl.ds(head, 1), :], rest], axis=1)
        band = pltpu.roll(jnp.broadcast_to(taps, (block, window)), 0, 1, stride=1, stride_axis=0)
        scales = jnp.concatenate([edge, scale_ref[pl.ds(scale_ref.shape[0] // 3 * 2 + head, 1), :], edge], axis=1)
        for start in starts:
            low, high = start - reach, start + block + reach
            pieces = [v_ref[max(low, 0) : min(high, tokens), there]]
            if low < 0:
                pieces = [blank] + pieces
            if high > tokens:
                pieces = pieces + [blank]
            values = jnp.concatenate(pieces, axis=0) if len(pieces) > 1 else pieces[0]
            weights = (band * scales[:, start : start + window]).astype(BF16)
            out_ref[start : start + block, there] = matmul(weights, values).astype(BF16)


def convolve(v, scales, taps):
    tokens, width = v.shape
    heads, tap_count = taps.shape
    reach = tap_count // 2
    per = heads_per_step(heads)
    block = 256 - 2 * reach
    starts = sorted(set(range(0, tokens - block, block)) | {tokens - block})
    return pl.pallas_call(
        functools.partial(conv_kernel, starts=starts, block=block),
        grid=(heads // per,),
        in_specs=[
            vmem(),
            vmem(),
            vmem(),
        ],
        out_specs=vmem(),
        out_shape=jax.ShapeDtypeStruct((tokens, width), BF16),
        compiler_params=params(limit=CONV_LIMIT),
        cost_estimate=cost(30_000_000_000),
        name="conv",
    )(v, scales, taps)


def landmark_softmax(q_marks, k_marks):
    scores = matmul(q_marks, k_marks, NT) * (FACTOR * LOG2E)
    weights = jnp.exp2(scores - jnp.max(scores, axis=1, keepdims=True))
    return weights / jnp.sum(weights, axis=1, keepdims=True)


def middle_kernel(here_ref, taps_ref, *refs, count, xor):
    pieces, (q_ref, k_ref, top_ref, before_ref, after_ref) = refs[:-5], refs[-5:]
    heads, tap_count = taps_ref.shape
    reach = tap_count // 2
    marks = (pieces[0].shape[0] - reach) // 2
    here = here_ref[0]
    for n in range(count):
        at = pl.multiple_of(source(here, n, xor) * marks, marks)
        q_ref[pl.ds(at, marks), :] = pieces[n][:marks, :]
        k_ref[pl.ds(at, marks), :] = pieces[n][marks : 2 * marks, :]
    line = lax.broadcasted_iota(jnp.int32, top_ref.shape, 0)
    rest = jnp.zeros((1, HEAD_DIM - tap_count), F32)
    odd = here % 2 == 1
    beyond = jnp.bitwise_xor(here, jnp.where(odd, here + 1, here - 1))
    tops = []
    for h in range(heads):
        at = slice(h * HEAD_DIM, (h + 1) * HEAD_DIM)
        middle = landmark_softmax(q_ref[:, at], k_ref[:, at])
        cols = jnp.sum(middle, axis=0, keepdims=True)
        cols = jnp.maximum(cols[:, :HEAD_DIM], cols[:, HEAD_DIM:])
        rows = jnp.max(jnp.sum(middle, axis=1, keepdims=True), axis=0, keepdims=True)
        tops.append(jnp.where(line == 0, cols, rows))
        if xor:
            beside = pieces[1][2 * marks :, at].astype(F32)
            across = jnp.zeros_like(beside)
            step = 4
            while step <= count:
                item = pieces[step - 1][2 * marks :, at].astype(F32)
                across = jnp.where(beyond == step - 1, item, across)
                step *= 2
            before = jnp.where(odd, beside, across).astype(BF16)
            after = jnp.where(odd, across, beside).astype(BF16)
        else:
            before, after = pieces[count][0, :, at], pieces[count][1, :, at]
        taps = jnp.concatenate([taps_ref[h : h + 1, :], rest], axis=1)
        band = jnp.broadcast_to(taps, (reach, HEAD_DIM))
        band = pltpu.roll(band, 0, 1, stride=1, stride_axis=0)
        low = band[:, :reach].astype(BF16)
        high = band[:, 2 * reach : 3 * reach].astype(BF16)
        before_ref[:, at] = matmul(low, before)
        after_ref[:, at] = matmul(high, after)
    top_ref[...] = functools.reduce(jnp.maximum, tops)


def middle_tops(here, taps, pieces, xor):
    width = pieces[0].shape[1]
    marks = jax.ShapeDtypeStruct((LANDMARKS, width), BF16)
    edge = jax.ShapeDtypeStruct((taps.shape[1] // 2, width), F32)
    return pl.pallas_call(
        functools.partial(middle_kernel, count=len(pieces) - (not xor), xor=xor),
        in_specs=[pl.BlockSpec(memory_space=pltpu.SMEM)] + [vmem()] * (1 + len(pieces)),
        out_specs=[vmem()] * 5,
        out_shape=[marks, marks, jax.ShapeDtypeStruct((8, HEAD_DIM), F32), edge, edge],
        compiler_params=params(False),
        name="middle",
    )(here, taps, *pieces)


def far_head(q_marks, keys, values, key_scale, value_scale):
    scores = matmul(q_marks, keys, NT) * (key_scale * (FACTOR * LOG2E))
    top = jnp.max(scores, axis=1, keepdims=True)
    weights = jnp.exp2(scores - top)
    total = jnp.sum(weights, axis=1, keepdims=True)
    weights = (weights * value_scale).astype(BF16)
    summed = matmul(weights, values) / total
    level = jnp.broadcast_to(top + jnp.log2(total), (LANDMARKS, HEAD_DIM))
    level = jnp.transpose(level)[:1, :]
    first = level.astype(BF16).astype(F32)
    second = (level - first).astype(BF16).astype(F32)
    third = level - first - second
    line = lax.broadcasted_iota(jnp.int32, (EXTRA, HEAD_DIM), 0)
    extra = jnp.zeros((EXTRA, HEAD_DIM), F32)
    for n, part in enumerate((first, second, third)):
        extra = jnp.where(line == 2 * n, part[:, :HEAD_DIM], extra)
        extra = jnp.where(line == 2 * n + 1, part[:, HEAD_DIM:], extra)
    return summed.astype(BF16), extra.astype(BF16)


def far_kernel(here_ref, q_ref, k_ref, v_ref, scale_ref, *out_refs, xor):
    step = pl.program_id(0)
    heads = scale_ref.shape[0] // 3
    per = heads_per_step(heads)
    results = []
    for u in range(per):
        head = source(here_ref[0], step * per + u, xor)
        at = pl.ds(pl.multiple_of(head * HEAD_DIM, HEAD_DIM), HEAD_DIM)
        scales = [scale_ref[pl.ds(n * heads + head, 1), :] for n in (1, 2)]
        results.append(far_head(q_ref[:, at], k_ref[:, at], v_ref[:, at], *scales))
    for n, out_ref in enumerate(out_refs):

        @pl.when(step == n // per)
        def _(out_ref=out_ref, result=results[n % per]):
            out_ref[:LANDMARKS, :] = result[0]
            out_ref[LANDMARKS:, :] = result[1]


def far_pieces(here, q_marks, k, v, scales, xor):
    heads = scales.shape[0] // 3
    per = heads_per_step(heads)
    shape = (LANDMARKS + EXTRA, HEAD_DIM)
    return pl.pallas_call(
        functools.partial(far_kernel, xor=xor),
        grid_spec=pltpu.PrefetchScalarGridSpec(
            num_scalar_prefetch=1,
            grid=(heads // per,),
            in_specs=[vmem()] * 4,
            out_specs=[vmem()] * heads,
        ),
        out_shape=[jax.ShapeDtypeStruct(shape, BF16)] * heads,
        compiler_params=params(),
        cost_estimate=cost(30_000_000_000),
        name="far",
    )(here, q_marks, k, v, scales)


def split(x):
    high = x.astype(BF16)
    return high, (x - high.astype(F32)).astype(BF16)


def fine(a, b):
    return matmul(a[0], b[0]) + (matmul(a[0], b[1]) + matmul(a[1], b[0]))


def newton_kernel(head_ref, q_ref, k_ref, *refs):
    tops, out_ref = refs[:-1], refs[-1]
    top = functools.reduce(jnp.maximum, [ref[...] for ref in tops])
    scale = jnp.max(top[0:1, :], axis=1, keepdims=True) * jnp.max(
        top[1:2, :], axis=1, keepdims=True
    )
    at = pl.ds(pl.multiple_of(head_ref[0] * HEAD_DIM, HEAD_DIM), HEAD_DIM)
    middle = landmark_softmax(q_ref[:, at], k_ref[:, at])
    iterate = jnp.transpose(middle) / scale
    middle = split(middle)
    coarse = lambda a, b: matmul(a[0], b[0])
    row = lax.broadcasted_iota(jnp.int32, (LANDMARKS, LANDMARKS), 0)
    col = lax.broadcasted_iota(jnp.int32, (LANDMARKS, LANDMARKS), 1)
    eye = jnp.where(row == col, 1.0, 0.0)
    for sweep in range(SWEEPS):
        product = coarse if sweep < COARSE else fine
        pair = split(iterate)
        whole = product(middle, pair)
        power = split(whole)
        inner = 7.0 * eye - whole
        inner = 15.0 * eye - product(power, split(inner))
        inner = 13.0 * eye - product(power, split(inner))
        iterate = 0.25 * product(pair, split(inner))
    out_ref[...] = iterate


def newton(head, q_marks, k_marks, tops):
    return pl.pallas_call(
        newton_kernel,
        in_specs=[pl.BlockSpec(memory_space=pltpu.SMEM)] + [vmem()] * (2 + len(tops)),
        out_specs=vmem(),
        out_shape=jax.ShapeDtypeStruct((LANDMARKS, LANDMARKS), F32),
        cost_estimate=cost(30_000_000_000),
        compiler_params=params(False),
        name="newton",
    )(head, q_marks, k_marks, *tops)


def apply_kernel(inverse_ref, *refs):
    pieces, out_ref = refs[:-1], refs[-1]
    count = len(pieces)
    levels = []
    for ref in pieces:
        extra = ref[LANDMARKS:, :].astype(F32)
        halves = [extra[n : n + 1] + extra[n + 2 : n + 3] + extra[n + 4 : n + 5] for n in (0, 1)]
        levels.append(jnp.concatenate(halves, axis=1))
    top = functools.reduce(jnp.maximum, levels)
    shares = [jnp.exp2(level - top) for level in levels]
    total = functools.reduce(jnp.add, shares)
    line = lax.broadcasted_iota(jnp.int32, (HEAD_DIM, LANDMARKS), 0)
    table = jnp.zeros((HEAD_DIM, LANDMARKS), F32)
    for n, share in enumerate(shares):
        table = jnp.where(line == n, share / total, table)
    table = jnp.transpose(table)
    reduced = jnp.zeros((LANDMARKS, HEAD_DIM), F32)
    for n in range(count):
        reduced = reduced + pieces[n][:LANDMARKS, :].astype(F32) * table[:, n : n + 1]
    out_ref[...] = fine(split(inverse_ref[...]), split(reduced)).astype(BF16)


def apply_inverse(inverse, pieces):
    return pl.pallas_call(
        apply_kernel,
        in_specs=[vmem()] * (1 + len(pieces)),
        out_specs=vmem(),
        out_shape=jax.ShapeDtypeStruct((LANDMARKS, HEAD_DIM), BF16),
        compiler_params=params(False),
        name="apply",
    )(inverse, *pieces)


def near_kernel(q_ref, scale_ref, marks_ref, out_ref, *, first, block):
    heads = scale_ref.shape[0] // 3
    rows = pl.ds(pl.multiple_of(pl.program_id(0) * block, block), block)
    scales = jnp.transpose(scale_ref[:heads, rows] * (FACTOR * LOG2E))
    for n in range(out_ref.shape[1] // LANDMARKS):
        at = slice((first + n) * HEAD_DIM, (first + n + 1) * HEAD_DIM)
        q = q_ref[rows, at]
        scores = matmul(q, marks_ref[:, at], NT)
        top = jnp.max(scores.astype(BF16), axis=1, keepdims=True).astype(F32)
        weights = jnp.exp2((scores - top) * scales[:, first + n : first + n + 1])
        out_ref[rows, n * LANDMARKS : (n + 1) * LANDMARKS] = weights.astype(BF16)


def near_weights(q, scales, k_marks, part, parts):
    tokens, width = q.shape
    here = scales.shape[0] // 3 // parts
    block = NEAR_BLOCK
    return pl.pallas_call(
        functools.partial(near_kernel, first=part * here, block=block),
        grid=(tokens // block,),
        in_specs=[vmem()] * 3,
        out_specs=vmem(),
        out_shape=jax.ShapeDtypeStruct((tokens, here * LANDMARKS), BF16),
        compiler_params=params(),
        cost_estimate=cost(30_000_000_000),
        name="near",
    )(q, scales, k_marks)


def final_kernel(here_ref, *refs, xor, parts):
    near, (conv_ref, before_ref, after_ref) = refs[:parts], refs[parts : parts + 3]
    mapped, (out_ref, table_ref) = refs[parts + 3 : -2], refs[-2:]
    heads = len(mapped)
    block, reach = out_ref.shape[0], before_ref.shape[0]
    step = pl.program_id(0)
    rows = pl.ds(pl.multiple_of(step * block, block), block)

    @pl.when(step == 0)
    def _():
        for n, ref in enumerate(mapped):
            head = source(here_ref[0], n, xor)
            table_ref[head, :, :HEAD_DIM] = ref[...]
            table_ref[head, :, HEAD_DIM:] = jnp.ones((LANDMARKS, HEAD_DIM), BF16)

    for h in range(heads):
        at = slice(h * HEAD_DIM, (h + 1) * HEAD_DIM)
        weights_ref = near[h * parts // heads]
        n = h % (heads // parts)
        weights = weights_ref[rows, n * LANDMARKS : (n + 1) * LANDMARKS]
        both = matmul(weights, table_ref[h])
        attended = both[:, :HEAD_DIM] / both[:, HEAD_DIM:]
        out_ref[:, at] = (attended + conv_ref[rows, at].astype(F32)).astype(BF16)

    @pl.when(step == 0)
    def _():
        out_ref[:reach, :] = (out_ref[:reach, :].astype(F32) + before_ref[...]).astype(BF16)

    @pl.when(step == pl.num_programs(0) - 1)
    def _():
        tail = slice(block - reach, block)
        out_ref[tail, :] = (out_ref[tail, :].astype(F32) + after_ref[...]).astype(BF16)


def finish(here, near, conv, before, after, mapped, xor):
    tokens, width = conv.shape
    block = FINAL_BLOCK
    heads, parts = len(mapped), len(near)
    return pl.pallas_call(
        functools.partial(final_kernel, xor=xor, parts=parts),
        grid=(tokens // block,),
        in_specs=[pl.BlockSpec(memory_space=pltpu.SMEM)] + [vmem()] * (parts + 3 + heads),
        out_specs=pl.BlockSpec((block, width), lambda t: (t, 0)),
        out_shape=jax.ShapeDtypeStruct((tokens, width), BF16),
        scratch_shapes=[pltpu.VMEM((heads, LANDMARKS, 2 * HEAD_DIM), BF16)],
        compiler_params=params(),
        name="finish",
    )(here, *near, conv, before, after, *mapped)


def shards(q_values, k_values, v_values, q_scales, k_scales, v_scales, conv_weight):
    tokens, width = q_values.shape
    heads, tap_count = conv_weight.shape
    reach = tap_count // 2
    seq_count, head_count = lax.axis_size("seq"), lax.axis_size("head")
    marks = LANDMARKS // seq_count
    xor = seq_count == heads and seq_count & (seq_count - 1) == 0
    position = lax.axis_index("seq").astype(jnp.int32)
    here = position.reshape(1)

    scales = jnp.concatenate([q_scales.T, k_scales.T, v_scales.T])
    means, means_near, q_keep, k_keep = landmark_means(
        here, q_values, k_values, v_values, scales, marks, reach, xor
    )
    mixed = convolve(v_values, scales, conv_weight)
    if xor:
        far = exchange_far(means, "seq", seq_count)
        far, mixed = lax.optimization_barrier((far, mixed))
        near = exchange_near([means_near] + far, "seq", seq_count)
        gathered = interleave([means] + far, near)
    else:
        up = [(i, i + 1) for i in range(seq_count - 1)]
        down = [(j, i) for i, j in up]
        before = lax.ppermute(means_near[2 * marks :], "seq", up)
        after = lax.ppermute(means[2 * marks :], "seq", down)
        gathered = gather_all(means, "seq", seq_count) + [jnp.stack([before, after])]
    q_marks, k_marks, top, before, after = middle_tops(here, conv_weight, gathered, xor)
    pieces = far_pieces(here, q_marks, k_keep, v_values, scales, xor)
    pieces, top = lax.optimization_barrier((pieces, top))
    if head_count & (head_count - 1) == 0 and head_count <= 4:
        tops = [top] + [
            lax.ppermute(top, "head", [(i, i ^ step) for i in range(head_count)])
            for step in range(1, head_count)
        ]
    else:
        tops = [lax.pmax(top, "head")]

    if xor:
        own_head = here
        pieces = [pieces[0]] + [
            lax.ppermute(pieces[step], "seq", [(i, i ^ step) for i in range(seq_count)])
            for step in range(1, seq_count)
        ]
    else:
        repeat = seq_count // heads
        own_head = here // repeat
        whole = lax.all_gather(jnp.stack(pieces), "seq", axis=0)
        mine = lax.dynamic_index_in_dim(whole, own_head[0], axis=1, keepdims=False)
        pieces = [mine[n] for n in range(seq_count)]

    inverse = newton(own_head, q_marks, k_marks, tops)
    mapped = apply_inverse(inverse, pieces)
    parts = heads_per_step(heads)
    near = [near_weights(q_keep, scales, k_marks, part, parts) for part in range(parts)]
    if xor:
        far = exchange_far(mapped, "seq", seq_count)
        far, near[0] = lax.optimization_barrier((far, near[0]))
        mapped = interleave([mapped] + far, exchange_near([mapped] + far, "seq", seq_count))
    else:
        mapped = gather_all(mapped, "seq", seq_count)[:: seq_count // heads]
    return finish(here, near, mixed, before, after, mapped, xor)


def solution(mesh):
    return jax.shard_map(
        shards,
        mesh=mesh,
        in_specs=(
            P("seq", "head"),
            P("seq", "head"),
            P("seq", "head"),
            P("seq", "head"),
            P("seq", "head"),
            P("seq", "head"),
            P("head", None),
        ),
        out_specs=P("seq", "head"),
        check_vma=False,
    )
```
